256 devices in a mesh: ex: 32 (over z, y), ckpt: 8 (over x, core).
Axes of the slice: x: 4, y: 4, z: 8, core: 2. Of those that a mesh axis runs over, the one named last changes fastest.
Arguments:
- grads: bfloat16 [8, 10240, 4096], P('ckpt', 'ex'), may hold values from -6 to 6
- second_moment: float32 [8, 4096], P('ckpt'), may hold values from 0.25 to 4
- step_size: float32 [8], P('ckpt'), may hold values from 0.25 to 1
- partners: int32 [32, 8], P('ex'), may hold values from -1 to 31, as said below
- counts: int32 [32], P('ex'), may hold values from 1 to 8, as said below
Outputs:
- band_rows: float32 [10240, 5120], P('ex', 'ckpt')
The draws below stay inside these ranges and needn't reach their ends.
Inputs may be any that keep to these rules, and one draw needn't show every extreme that they name: For s < counts[b], partners[b, s] are distinct blocks among (b + 1) mod 32 to (b + 8) mod 32; slots from counts[b] on hold -1. `counts`: some block has 8 live slots in every draw.
All inputs are finite; a program needn't handle non-finite values.
Results may differ from the reference program's by a relative error of at most 0.0029.
Values may be sent and summed in bfloat16 or wider, within the bound.
No kernel may reach another device: no remote copies, remote signals or barrier semaphores. Data moves between devices by JAX's collectives and lax.ppermute only.
A program may use at most 64 MiB of HBM per device.

```python
import math
import jax
import jax.numpy as jnp
from jax import lax

P_SIZE = 4096
BR = 320
CKPT = 8
BLOCKS = 32
EXAMPLES = 10240
REACH = 8


def pair_layout(key):
    base = jax.random.fold_in(key, 7)
    first_key, second_key, third_key = jax.random.split(base, 3)
    shifts = jax.random.randint(first_key, (BLOCKS,), 0, 4)
    amounts = jnp.maximum(jnp.right_shift(jnp.int32(REACH), shifts.astype(jnp.int32)), 1)
    busiest = jax.random.randint(second_key, (), 0, BLOCKS)
    amounts = jnp.where(jnp.arange(BLOCKS) == busiest, REACH, amounts).astype(jnp.int32)
    row_keys = jax.random.split(third_key, BLOCKS)
    orders = jax.vmap(lambda row_key: jax.random.permutation(row_key, REACH))(row_keys).astype(jnp.int32) + 1
    partner_ids = jnp.mod(jnp.arange(BLOCKS, dtype=jnp.int32)[:, None] + orders, BLOCKS)
    alive_slot = jnp.arange(REACH, dtype=jnp.int32)[None, :] < amounts[:, None]
    partner_ids = jnp.where(alive_slot, partner_ids, -1).astype(jnp.int32)
    return (partner_ids, amounts)


def draw_partners(key, part):
    return pair_layout(key)[0]


def draw_counts(key, part):
    return pair_layout(key)[1]


def steps_of(rng, extent, cuts, low, largest):
    level = 1.0
    for position, shards_of in cuts:
        heights = jax.random.uniform(jax.random.fold_in(jax.random.fold_in(rng, 6), position), (shards_of,), jnp.float32, low / len(cuts), largest / len(cuts))
        level = level * jnp.repeat(jnp.exp(heights), extent[position] // shards_of).reshape((-1,) + (1,) * (len(extent) - 1 - position))
    return level


def scatter_about(rng, dims, deviation, most, shards=(), kind=jnp.bfloat16):
    level = steps_of(rng, dims, shards, -0.22, 0.18) if shards else 1.0
    array = jax.random.normal(rng, dims, jnp.float32) * deviation * level
    return jnp.minimum(jnp.maximum(array, -most), most).astype(kind)


def setup_inputs(seed: int = 0) -> dict:
    streams_of = jax.random.split(jax.random.key(seed), 6)
    grads = scatter_about(streams_of[0], (CKPT, EXAMPLES, P_SIZE), 1.0, 6.0, ((0, 8), (1, 32)))
    second_moment = jnp.clip(jnp.exp(math.log(4.0) - 2.7725887 * jax.random.uniform(streams_of[1], (CKPT, P_SIZE), jnp.float32) ** steps_of(streams_of[1], (CKPT, P_SIZE), ((0, 8),), -0.2, 0.2)), 0.25, 4.0)
    step_size = jnp.clip(jnp.exp(math.log(1.0) - 1.3862944 * jax.random.uniform(streams_of[2], (CKPT,), jnp.float32) ** steps_of(streams_of[2], (CKPT,), ((0, 8),), -0.2, 0.2)), 0.25, 1.0)
    partners = draw_partners(jax.random.fold_in(streams_of[5], 71), 0)
    counts = draw_counts(jax.random.fold_in(streams_of[5], 71), 0)
    return dict(grads=grads, second_moment=second_moment, step_size=step_size, partners=partners, counts=counts)


EPSILON = 1e-08

def reference(grads, second_moment, step_size, partners, counts):
    factor = step_size[:, None] / (jnp.sqrt(second_moment) + EPSILON) * P_SIZE ** (-0.5)
    scaled = (grads.astype(jnp.float32) * factor[:, None, :]).astype(jnp.bfloat16)
    blocks = BLOCKS
    alive_slot = jnp.arange(REACH, dtype=jnp.int32)[None, :] < counts[:, None]
    offsets = jnp.mod(partners - jnp.arange(blocks, dtype=jnp.int32)[:, None], blocks)
    left_side = scaled.reshape(CKPT, blocks, BR, P_SIZE)
    right_side = grads.reshape(CKPT, blocks, BR, P_SIZE)
    forward = []
    backward = []
    for offset in range(1, REACH + 1):
        matched = jnp.logical_and(offsets == offset, alive_slot)
        listed = lax.optimization_barrier(jnp.sum(matched.astype(jnp.int32), axis=1))
        partner_rows = jnp.roll(right_side, -offset, axis=1)

        def add_checkpoint(running, operands):
            product = jnp.einsum('nrp,nsp->nrs', operands[0].astype(jnp.float32), operands[1].astype(jnp.float32))
            return (running + product, None)
        tile_set, unused = lax.scan(add_checkpoint, jnp.zeros((blocks, BR, BR), jnp.float32), (left_side, partner_rows))
        tile_set = tile_set * listed.astype(jnp.float32)[:, None, None]
        forward.append(tile_set)
        backward.insert(0, jnp.transpose(jnp.roll(tile_set, offset, axis=0), (0, 2, 1)))
    band_rows = jnp.stack(backward + forward, axis=2)
    return band_rows.reshape(blocks * BR, 2 * REACH * BR)
```

```python
import jax
import jax.numpy as jnp
from jax import lax
from jax.sharding import PartitionSpec as P

EPSILON = 1e-08
AXES = ("ex", "ckpt")
NY = 4


def local_fn(planes):
    span = planes * NY

    def flat(z, y, x, c):
        return ((z % planes) * NY + y % NY) * 8 + (x % 4) * 2 + c

    def perm(move):
        pairs = []
        for z in range(planes):
            for y in range(NY):
                for x in range(4):
                    for c in range(2):
                        target = move(z, y, x, c)
                        if target is not None:
                            pairs.append((flat(z, y, x, c), flat(*target)))
        return pairs

    def send(value, move):
        return lax.ppermute(value, AXES, perm(move))

    def local(grads, second_moment, step_size, partners, counts):
        width = grads.shape[2]
        rows = grads.shape[1]
        reach = partners.shape[1]
        quarter = width // NY
        half = rows // 2
        e = lax.axis_index("ex")
        k = lax.axis_index("ckpt")
        y = lax.rem(e, NY)
        x = k // 2
        c = lax.rem(k, 2)
        own = grads[0]

        def cut(index):
            return lax.dynamic_slice_in_dim(own, lax.rem(index, NY) * quarter, quarter, 1)

        offsets = jnp.mod(partners[0] - e, span)
        alive = jnp.arange(reach, dtype=jnp.int32) < counts[0]
        wanted = jnp.arange(1, reach + 1, dtype=jnp.int32)
        matched = jnp.logical_and(offsets[:, None] == wanted[None, :], alive[:, None])
        listed = jnp.sum(matched.astype(jnp.float32), axis=0)
        before = send(listed, lambda z, y, x, c: (z + 1, y, x, c))
        lists = jnp.stack([listed, before])

        pieces = [None] * NY
        pieces[0] = cut(y)
        for s in (1, 3, 2):
            pieces[NY - s] = send(cut(y + s), lambda z, y, x, c, s=s: (z, y + s, x, c))
        above = [None] * NY
        below = [None] * NY
        for r in (0, 3, 1, 2):
            above[r] = send(pieces[r], lambda z, y, x, c: (z - 1, y, x, c))
            below[r] = send(pieces[r], lambda z, y, x, c: (z + 1, y, x, c))

        factor = step_size[:, None] / (jnp.sqrt(second_moment) + EPSILON) * width ** (-0.5)
        factor = lax.dynamic_slice_in_dim(factor, y * quarter, quarter, 1)

        def scale(piece):
            return (piece.astype(jnp.float32) * factor).astype(jnp.bfloat16)

        here = [scale(piece) for piece in pieces]
        early = [scale(piece) for piece in below]

        def dot(left, right):
            return lax.dot_general(left, right, (((1,), (1,)), ((), ())), preferred_element_type=jnp.float32)

        column_beta = NY - jnp.arange(NY * rows, dtype=jnp.int32) // rows
        kept, given = [], []
        for r in range(NY):
            order = [(r - beta) % NY for beta in (4, 3, 2, 1)]
            now = jnp.concatenate([here[s] for s in order], axis=0)
            ago = jnp.concatenate([early[s] for s in order], axis=0)
            inside = dot(pieces[r], now)
            across = dot(above[r], now)
            beyond = dot(above[r], ago)
            wrap = (lax.rem(y + r, NY) < column_beta)[None, :]
            both = jnp.stack([jnp.where(wrap, across, inside), jnp.where(wrap, beyond, across)])
            kept.append(lax.dynamic_slice_in_dim(both, (1 - c) * 2 * rows, 2 * rows, 2))
            given.append(lax.dynamic_slice_in_dim(both, c * 2 * rows, 2 * rows, 2).astype(jnp.bfloat16))
        kept = jnp.stack(kept, axis=1)
        given = jnp.stack(given, axis=1)
        total = kept + send(given, lambda z, y, x, c: (z, y, x, 1 - c)).astype(jnp.float32)

        def share(at):
            at = lax.rem(at, 4)
            kind = jnp.where(jnp.logical_or(at == 0, at == 3), 1, 0)
            part = jnp.where(at >= 2, 1, 0)
            return lax.dynamic_slice(total, (kind, 0, part * half, 0), (1, NY, half, 2 * rows))[0]

        summed = share(x)
        for t in (1, 3, 2):
            arrived = send(share(x + t).astype(jnp.bfloat16), lambda z, y, x, c, t=t: (z, y, x + t, c))
            summed = summed + arrived.astype(jnp.float32)

        final = summed[0]
        for r in (1, 3, 2):
            arrived = send(summed[r].astype(jnp.bfloat16), lambda z, y, x, c, r=r: (z, y + r, x, c))
            final = final + arrived.astype(jnp.float32)

        around = [lists] + [send(lists, lambda z, y, x, c, s=s: (z, y + s, x, c)) for s in (1, 2, 3)]
        around = jnp.stack(around)
        is_far = jnp.logical_or(x == 0, x == 3)
        weights = []
        for beta in (2 * c + 2, 2 * c + 1):
            wrap = y < beta
            source = around[lax.rem(beta, NY)]
            plane = jnp.where(jnp.logical_and(is_far, wrap), source[1], source[0])
            weights.append(plane[beta - 1 + jnp.where(is_far, NY, 0)])
        weight = jnp.where(jnp.arange(2 * rows) < rows, weights[0], weights[1])[None, :]
        final = jnp.where(weight > 0, final, 0.0)

        def betas(c):
            return (2 * c + 2, 2 * c + 1)

        def back(first, up):
            def move(z, y, x, c):
                if (x < 2) != first:
                    return None
                far = x in (0, 3)
                if far:
                    return (z + 1, y, 0, 1 - c) if up else None
                needed = any((y < beta) == up for beta in betas(c))
                return (z + up, y, 1, 1 - c) if needed else None

            return move

        same = jnp.concatenate([send(final, back(True, False)), send(final, back(False, False))], axis=0)
        upper = jnp.concatenate([send(final, back(True, True)), send(final, back(False, True))], axis=0)
        arrived_beta = jnp.where(jnp.arange(2 * rows) < rows, 2 * (1 - c) + 2, 2 * (1 - c) + 1)
        take = jnp.logical_or(x == 0, y < arrived_beta)[None, :]
        backward = jnp.where(take, upper, same)

        def ahead(first, which):
            def move(z, y, x, c):
                if (x < 2) != first:
                    return None
                beta = betas(c)[which]
                far = x in (0, 3)
                down = 1 if far and y < beta else 0
                return (z - down, y - beta, 3 if far else 2, c)

            return move

        columns = []
        for which in (1, 0):
            tile = final[:, which * rows : (which + 1) * rows]
            whole = jnp.concatenate([send(tile, ahead(True, which)), send(tile, ahead(False, which))], axis=0)
            columns.append(whole.T)
        forward = jnp.concatenate(columns, axis=1)
        return jnp.where(x >= 2, forward, backward)

    return local


def solution(mesh):
    local = local_fn(mesh.shape["ex"] // NY)
    in_specs = (P("ckpt", "ex", None), P("ckpt", None), P("ckpt"), P("ex", None), P("ex"))
    return jax.shard_map(local, mesh=mesh, in_specs=in_specs, out_specs=P("ex", "ckpt"), check_vma=False)
```

```python
import jax
import jax.numpy as jnp
from jax import lax
from jax.experimental import pallas as pl
from jax.experimental.pallas import tpu as pltpu
from jax.sharding import PartitionSpec as P


EPSILON = 1e-08
AXES = ("ex", "ckpt")
NY = 4
CHUNK = 32


def tiles_kernel(place_ref, factor_ref, *refs):
    here, above, below = refs[0:4], refs[4:8], refs[8:12]
    keep_ref, give_ref, left_ref, right_ref = refs[12:]
    rows = here[0].shape[0]
    half = rows // 2
    y = place_ref[0]
    c = place_ref[1]
    r = pl.program_id(0)

    @pl.when(r == 0)
    def _():
        for plane, group in enumerate((below, here, above)):
            for rel in range(NY):
                start = (plane * NY + lax.rem(y + rel, NY)) * rows

                @pl.loop(0, rows // CHUNK)
                def _(step, plane=plane, group=group, rel=rel, start=start):
                    source = pl.ds(pl.multiple_of(step * CHUNK, CHUNK), CHUNK)
                    target = pl.ds(pl.multiple_of(start + step * CHUNK, CHUNK), CHUNK)
                    piece = group[rel][source, :]
                    left_ref[target, :] = (piece.astype(jnp.float32) * factor_ref[...]).astype(jnp.bfloat16)
                    if plane == 2:
                        right_ref[rel, source, :] = piece

    b = lax.rem(y + r, NY)
    for far in range(2):
        for out_ref, core in ((keep_ref, c), (give_ref, 1 - c)):
            start = pl.multiple_of((b + 6 - 2 * (2 * far + core)) * rows, CHUNK)
            product = lax.dot_general(
                right_ref[r],
                left_ref[pl.ds(start, 2 * rows), :],
                (((1,), (1,)), ((), ())),
                preferred_element_type=jnp.float32,
            ).astype(out_ref.dtype)
            low, high = (0, 3) if far else (1, 2)
            for slot, first in ((high, 0), (low, rows)):
                out_ref[0, slot, :, 0:rows] = product[0:half, first : first + rows]
                out_ref[0, slot, :, rows : 2 * rows] = product[half:rows, first : first + rows]


def tiles(place, factor, here, above, below):
    rows, width = here[0].shape
    half = rows // 2
    vmem = pl.BlockSpec(memory_space=pltpu.VMEM)
    block = pl.BlockSpec((1, 4, half, 2 * rows), lambda r: (r, 0, 0, 0))
    return pl.pallas_call(
        tiles_kernel,
        grid=(NY,),
        in_specs=[pl.BlockSpec(memory_space=pltpu.SMEM), vmem] + [vmem] * 12,
        out_specs=[block, block],
        out_shape=[
            jax.ShapeDtypeStruct((NY, 4, half, 2 * rows), jnp.float32),
            jax.ShapeDtypeStruct((NY, 4, half, 2 * rows), jnp.bfloat16),
        ],
        scratch_shapes=[
            pltpu.VMEM((3 * NY * rows, width), jnp.bfloat16),
            pltpu.VMEM((NY, rows, width), jnp.bfloat16),
        ],
        compiler_params=pltpu.CompilerParams(vmem_limit_bytes=44 * 2**20),
        cost_estimate=pl.CostEstimate(
            flops=2 * 32 * rows * rows * width, bytes_accessed=24 * rows * width * 2, transcendentals=0
        ),
    )(place, factor, *here, *above, *below)


def local_fn(blocks):
    def flat(e, x, c):
        return (e % blocks) * 8 + (x % 4) * 2 + c

    def ring(e, by):
        return e - e % NY + (e + by) % NY

    def send(value, move):
        pairs = []
        for e in range(blocks):
            for x in range(4):
                for c in range(2):
                    target = move(e, x, c)
                    if target is not None:
                        pairs.append((flat(e, x, c), flat(*target)))
        return lax.ppermute(value, AXES, pairs)

    def offset_of(x, c):
        return (4 if x in (0, 3) else 0) + 2 * c + 1 + (1 if x >= 2 else 0)

    def local(grads, second_moment, step_size, partners, counts):
        width = grads.shape[2]
        rows = grads.shape[1]
        reach = partners.shape[1]
        quarter = width // NY
        part = rows // 4
        e = lax.axis_index("ex")
        k = lax.axis_index("ckpt")
        y = lax.rem(e, NY)
        x = k // 2
        c = lax.rem(k, 2)
        own = grads[0]

        def cut(index):
            return lax.dynamic_slice_in_dim(own, lax.rem(index, NY) * quarter, quarter, 1)

        here = [None] * NY
        above = [None] * NY
        below = [None] * NY
        here[0] = lax.optimization_barrier(cut(y))
        for s in (1, 3, 2):
            here[NY - s] = send(cut(y + s), lambda e, x, c, s=s: (ring(e, s), x, c))
        for r in (0, 3, 1, 2):
            above[r] = send(here[r], lambda e, x, c: (e - NY, x, c))
            below[r] = send(here[r], lambda e, x, c: (e + NY, x, c))

        offsets = jnp.mod(partners[0] - e, blocks)
        alive = jnp.arange(reach, dtype=jnp.int32) < counts[0]
        wanted = jnp.arange(1, reach + 1, dtype=jnp.int32)
        matched = jnp.logical_and(offsets[:, None] == wanted[None, :], alive[:, None])
        listed = jnp.sum(matched.astype(jnp.float32), axis=0)
        listed = send(listed, lambda e, x, c: (e + offset_of(x, c) - NY, x, c))
        is_far = jnp.logical_or(x == 0, x == 3)
        offset = jnp.where(is_far, NY, 0) + 2 * c + 1 + jnp.where(x >= 2, 1, 0)
        weight = lax.dynamic_slice_in_dim(listed, offset - 1, 1, 0)[0]

        factor = step_size[:, None] / (jnp.sqrt(second_moment) + EPSILON) * width ** (-0.5)
        factor = lax.dynamic_slice_in_dim(factor, y * quarter, quarter, 1)
        keep, give = tiles(jnp.stack([y, c]), factor, here, above, below)

        given = send(give, lambda e, x, c: (e, x, 1 - c))
        total = keep + given.astype(jnp.float32)

        def pick(array, index, axis):
            return lax.dynamic_index_in_dim(array, lax.rem(index, 4), axis, keepdims=False)

        upper, lower = total[:, :, :part], total[:, :, part:]
        near_x = pick(upper, x, 1)
        near_y = lower[0]
        arrived_x, arrived_y = [], []
        for t in (1, 3, 2):
            arrived_x.append(send(pick(upper, x + t, 1).astype(jnp.bfloat16), lambda e, x, c, t=t: (e, x + t, c)))
            arrived_y.append(send(lower[t].astype(jnp.bfloat16), lambda e, x, c, t=t: (ring(e, t), x, c)))
        for value in arrived_x:
            near_x = near_x + value.astype(jnp.float32)
        for value in arrived_y:
            near_y = near_y + value.astype(jnp.float32)
        first = near_x[0]
        last = pick(near_y, x, 0)
        arrived_x, arrived_y = [], []
        for t in (1, 3, 2):
            arrived_y.append(send(near_x[t].astype(jnp.bfloat16), lambda e, x, c, t=t: (ring(e, t), x, c)))
            arrived_x.append(send(pick(near_y, x + t, 0).astype(jnp.bfloat16), lambda e, x, c, t=t: (e, x + t, c)))
        for value in arrived_y:
            first = first + value.astype(jnp.float32)
        for value in arrived_x:
            last = last + value.astype(jnp.float32)
        final = jnp.concatenate([first, last], axis=0)
        final = jnp.where(weight > 0, final, 0.0)

        def back(low):
            def move(e, x, c):
                if (x < 2) != low:
                    return None
                return (e + NY, 0 if x in (0, 3) else 1, 1 - c)

            return move

        def ahead(low):
            def move(e, x, c):
                if (x < 2) != low:
                    return None
                return (e + NY - offset_of(x, c), 3 if x in (0, 3) else 2, c)

            return move

        back_low = send(final, back(True))
        back_high = send(final, back(False))
        ahead_low = send(final, ahead(True))
        ahead_high = send(final, ahead(False))

        def later(tile):
            return jnp.concatenate([tile[:, :rows], tile[:, rows:]], axis=0)

        backward = jnp.concatenate([later(back_high), later(back_low)], axis=1)
        forward = jnp.concatenate([later(ahead_low), later(ahead_high)], axis=0)
        forward = jnp.concatenate([forward[:rows].T, forward[rows:].T], axis=1)
        return jnp.where(x >= 2, forward, backward)

    return local


def build(mesh):
    local = local_fn(mesh.shape["ex"])
    in_specs = (P("ckpt", "ex", None), P("ckpt", None), P("ckpt"), P("ex", None), P("ex"))
    return jax.shard_map(local, mesh=mesh, in_specs=in_specs, out_specs=P("ex", "ckpt"), check_vma=False)


def solution(mesh):
    return build(mesh)
```

```python
import functools

import jax
import jax.numpy as jnp
from jax import lax
from jax.experimental import pallas as pl
from jax.experimental.pallas import tpu as pltpu
from jax.sharding import PartitionSpec as P


EPSILON = 1e-08
AXES = ("ex", "ckpt")
NY = 4
CHUNK = 32


def scale_into(left_ref, piece_ref, factor_ref, start):
    @pl.loop(0, piece_ref.shape[0] // CHUNK)
    def _(step):
        source = pl.ds(pl.multiple_of(step * CHUNK, CHUNK), CHUNK)
        target = pl.ds(pl.multiple_of(start + step * CHUNK, CHUNK), CHUNK)
        piece = piece_ref[source, :].astype(jnp.float32)
        left_ref[target, :] = (piece * factor_ref[...]).astype(jnp.bfloat16)


def fill(out_ref, index, tile):
    half = tile.shape[0] // 2
    rows = tile.shape[1]
    out_ref[index, :, 0:rows] = tile[:half].astype(out_ref.dtype)
    out_ref[index, :, rows : 2 * rows] = tile[half:].astype(out_ref.dtype)


def product_of(right, left):
    return lax.dot_general(right, left, (((1,), (1,)), ((), ())), preferred_element_type=jnp.float32)


def owner(far, p):
    return jnp.where(far == 1, 3 * p, 1 + p)


def tiles_kernel(late, place_ref, factor_ref, *refs):
    if late:
        right_in, last_below, left_in = refs[0:4], refs[4], refs[5]
        keep_ref, give_ref, right_ref, left_ref, piece_ref, sems = refs[6:]
        loads = [(right_in[rel], right_ref.at[rel]) for rel in (2, 0, 1, 3)]
        loads += [(last_below, piece_ref.at[0]), (left_in, left_ref)]
    else:
        right_in, rest = refs[0:3], refs[3:10]
        left_out, keep_ref, give_ref, right_ref, left_ref, piece_ref, sems = refs[10:]
        loads = [(ref, right_ref.at[rel]) for rel, ref in zip((0, 1, 3), right_in)]
        loads += [(ref, piece_ref.at[i]) for i, ref in enumerate(rest)]
    rows = right_ref.shape[1]
    y = place_ref[0]
    c = place_ref[1]
    copies = [pltpu.make_async_copy(source, target, sems.at[i]) for i, (source, target) in enumerate(loads)]
    for copy in copies:
        copy.start()
    for copy in copies:
        copy.wait()
    if late:
        groups = ((0, 2, piece_ref.at[0]), (2, 2, right_ref.at[2]))
    else:
        groups = tuple((2, rel, right_ref.at[rel]) for rel in (0, 1, 3))
        groups += tuple((1, rel, piece_ref.at[rel]) for rel in range(NY))
        groups += tuple((0, rel, piece_ref.at[NY + i]) for i, rel in enumerate((0, 1, 3)))
    for plane, rel, ref in groups:
        scale_into(left_ref, ref, factor_ref, (plane * NY + lax.rem(y + rel, NY)) * rows)
    if not late:
        store = pltpu.make_async_copy(left_ref, left_out, sems.at[len(loads)])
        store.start()

    def start_of(r, offset):
        return pl.multiple_of((lax.rem(y + r, NY) + 2 * NY - offset) * rows, CHUNK)

    @pl.loop(0, 4)
    def _(turn):
        far = turn // 2
        given = lax.rem(turn, 2)
        core = jnp.where(given == 1, 1 - c, c)
        lowest = 4 * far + 2 * core + 1

        def one(slot, r, p):
            tile = product_of(right_ref[r], left_ref[pl.ds(start_of(r, lowest + p), rows), :])
            place(slot, p, tile)

        def place(slot, p, tile):
            index = slot * 4 + owner(far, p) if late else owner(far, p) * 2 + slot

            @pl.when(given == 0)
            def _():
                fill(keep_ref, index, tile)

            @pl.when(given == 1)
            def _():
                fill(give_ref, index, tile)

        if late:
            pair = product_of(right_ref[2], left_ref[pl.ds(start_of(2, lowest + 1), 2 * rows), :])
            place(0, 1, pair[:, :rows])
            place(0, 0, pair[:, rows:])
            one(1, jnp.where(core == 0, 3, 1), 0)
            one(1, 0, 1)
        else:
            one(0, 0, 0)
            one(0, 3, 1)
            one(1, jnp.where(core == 0, 1, 3), 0)
            one(1, 1, 1)

    if not late:
        store.wait()


def tiles(late, place, factor, *arrays):
    rows, width = arrays[0].shape
    half = rows // 2
    vmem = pl.BlockSpec(memory_space=pltpu.VMEM)
    hbm = pl.BlockSpec(memory_space=pltpu.HBM)
    left = [] if late else [jax.ShapeDtypeStruct((3 * NY * rows, width), jnp.bfloat16)]
    shapes = left + [
        jax.ShapeDtypeStruct((8, half, 2 * rows), jnp.float32),
        jax.ShapeDtypeStruct((8, half, 2 * rows), jnp.bfloat16),
    ]
    *left, keep, give = pl.pallas_call(
        functools.partial(tiles_kernel, late),
        in_specs=[pl.BlockSpec(memory_space=pltpu.SMEM), vmem] + [hbm] * len(arrays),
        out_specs=[hbm] * len(left) + [vmem] * 2,
        out_shape=shapes,
        scratch_shapes=[
            pltpu.VMEM((NY, rows, width), jnp.bfloat16),
            pltpu.VMEM((3 * NY * rows, width), jnp.bfloat16),
            pltpu.VMEM((1 if late else 7, rows, width), jnp.bfloat16),
            pltpu.SemaphoreType.DMA((11,)),
        ],
        compiler_params=pltpu.CompilerParams(vmem_limit_bytes=26 * 2**20),
        cost_estimate=pl.CostEstimate(
            flops=32 * rows * rows * width, bytes_accessed=12 * rows * width * 2, transcendentals=0
        ),
    )(place, factor, *arrays)
    shape = (2, 4, half, 2 * rows) if late else (4, 2, half, 2 * rows)
    return (*left, keep.reshape(shape), give.reshape(shape))


def local_fn(blocks):
    def flat(e, x, c):
        return (e % blocks) * 8 + (x % 4) * 2 + c

    def ring(e, by):
        return e - e % NY + (e + by) % NY

    def send(value, move):
        pairs = []
        for e in range(blocks):
            for x in range(4):
                for c in range(2):
                    target = move(e, x, c)
                    if target is not None:
                        pairs.append((flat(e, x, c), flat(*target)))
        return lax.ppermute(value, AXES, pairs)

    def offset_of(x, c):
        return (4 if x in (0, 3) else 0) + 2 * c + 1 + (1 if x >= 2 else 0)

    def local(grads, second_moment, step_size, partners, counts):
        width = grads.shape[2]
        rows = grads.shape[1]
        reach = partners.shape[1]
        quarter = width // NY
        part = rows // 4
        e = lax.axis_index("ex")
        k = lax.axis_index("ckpt")
        y = lax.rem(e, NY)
        x = k // 2
        c = lax.rem(k, 2)
        own = grads[0]

        def cut(index):
            return lax.dynamic_slice_in_dim(own, lax.rem(index, NY) * quarter, quarter, 1)

        here = [None] * NY
        above = [None] * NY
        below = [None] * NY
        here[0] = lax.optimization_barrier(cut(y))
        for s in (1, 3, 2):
            here[NY - s] = send(cut(y + s), lambda e, x, c, s=s: (ring(e, s), x, c))
        for r in (0, 3, 1, 2):
            above[r] = send(here[r], lambda e, x, c: (e - NY, x, c))
            below[r] = send(here[r], lambda e, x, c: (e + NY, x, c))

        offsets = jnp.mod(partners[0] - e, blocks)
        alive = jnp.arange(reach, dtype=jnp.int32) < counts[0]
        wanted = jnp.arange(1, reach + 1, dtype=jnp.int32)
        matched = jnp.logical_and(offsets[:, None] == wanted[None, :], alive[:, None])
        listed = jnp.sum(matched.astype(jnp.float32), axis=0)
        listed = send(listed, lambda e, x, c: (e + offset_of(x, c) - NY, x, c))
        is_far = jnp.logical_or(x == 0, x == 3)
        offset = jnp.where(is_far, NY, 0) + 2 * c + 1 + jnp.where(x >= 2, 1, 0)
        weight = lax.dynamic_slice_in_dim(listed, offset - 1, 1, 0)[0]

        factor = step_size[:, None] / (jnp.sqrt(second_moment) + EPSILON) * width ** (-0.5)
        factor = lax.dynamic_slice_in_dim(factor, y * quarter, quarter, 1)
        place = jnp.stack([y, c])
        left, keep, give = tiles(
            False, place, factor, above[0], above[1], above[3], *here, below[0], below[1], below[3]
        )

        def low_of(x):
            return x < 2

        def pick(array, index, axis):
            return lax.dynamic_index_in_dim(array, lax.rem(index, 4), axis, keepdims=False)

        def narrow(value):
            return value.astype(jnp.bfloat16)

        def wide(value):
            return value.astype(jnp.float32)

        given = send(give, lambda e, x, c: (e, x, 1 - c))
        total = keep + wide(given)
        early = pick(total, x, 0)
        arrived_early = [send(narrow(pick(total, x + t, 0)), lambda e, x, c, t=t: (e, x + t, c)) for t in (1, 3, 2)]
        keep, give = tiles(True, place, factor, *above, below[2], left)
        given = send(give, lambda e, x, c: (e, x, 1 - c))
        total = keep + wide(given)

        def rest(e, c):
            return ring(e, 3 if c == 0 else 1)

        upper, lower = total[:, :, :part], total[:, :, part:]
        by2 = send(narrow(lower[0]), lambda e, x, c: (ring(e, 2), x, c))
        by1 = send(narrow(lower[1, :2]), lambda e, x, c: (rest(e, c), x, c))
        upper_own = pick(upper, x, 1)
        arrived = [send(narrow(pick(upper, x + t, 1)), lambda e, x, c, t=t: (e, x + t, c)) for t in (1, 3, 2)]
        arrived_early, arrived[0] = lax.optimization_barrier((arrived_early, arrived[0]))
        for value in arrived_early:
            early = early + wide(value)
        low = low_of(x)
        final = jnp.where(low, early[0], 0.0)
        final = final + wide(send(narrow(early[1]), lambda e, x, c: (ring(e, 3 if low_of(x) and c == 1 else 1), x, c)))
        final = final + wide(send(narrow(early[0]), lambda e, x, c: None if low_of(x) else (ring(e, 3), x, c)))
        lower_own = wide(by2) + jnp.concatenate([wide(by1), lower[1, 2:]], axis=0)
        bottom = pick(lower_own, x, 0)
        bottom_arrived = [
            send(narrow(pick(lower_own, x + t, 0)), lambda e, x, c, t=t: (e, x + t, c)) for t in (1, 3, 2)
        ]
        for value in arrived:
            upper_own = upper_own + wide(value)
        ay2 = send(narrow(upper_own[0]), lambda e, x, c: (ring(e, 2), x, c))
        ay1 = send(narrow(upper_own[1]), lambda e, x, c: (rest(e, c), x, c) if low_of(x) else None)
        top = jnp.where(low, 0.0, upper_own[1]) + wide(ay2) + wide(ay1)
        for value in bottom_arrived:
            bottom = bottom + wide(value)
        final = final + jnp.concatenate([top, bottom], axis=0)
        final = jnp.where(weight > 0, final, 0.0)

        def back(low):
            def move(e, x, c):
                if (x < 2) != low:
                    return None
                return (e + NY, 0 if x in (0, 3) else 1, 1 - c)

            return move

        def ahead(low):
            def move(e, x, c):
                if (x < 2) != low:
                    return None
                return (e + NY - offset_of(x, c), 3 if x in (0, 3) else 2, c)

            return move

        back_low = send(final, back(True))
        back_high = send(final, back(False))
        ahead_low = send(final, ahead(True))
        ahead_high = send(final, ahead(False))

        def later(tile):
            return jnp.concatenate([tile[:, :rows], tile[:, rows:]], axis=0)

        backward = jnp.concatenate([later(back_high), later(back_low)], axis=1)
        forward = jnp.concatenate([later(ahead_low), later(ahead_high)], axis=0)
        forward = jnp.concatenate([forward[:rows].T, forward[rows:].T], axis=1)
        return jnp.where(x >= 2, forward, backward)

    return local


def build(mesh):
    local = local_fn(mesh.shape["ex"])
    in_specs = (P("ckpt", "ex", None), P("ckpt", None), P("ckpt"), P("ex", None), P("ex"))
    return jax.shard_map(local, mesh=mesh, in_specs=in_specs, out_specs=P("ex", "ckpt"), check_vma=False)


def solution(mesh):
    return build(mesh)
```

```python
import functools

import jax
import jax.numpy as jnp
from jax import lax
from jax.experimental import pallas as pl
from jax.experimental.pallas import tpu as pltpu
from jax.sharding import PartitionSpec as P


EPSILON = 1e-08
AXES = ("ex", "ckpt")
NY = 4
CHUNK = 32


def scale_into(left_ref, piece_ref, factor_ref, start):
    @pl.loop(0, piece_ref.shape[0] // CHUNK)
    def _(step):
        source = pl.ds(pl.multiple_of(step * CHUNK, CHUNK), CHUNK)
        target = pl.ds(pl.multiple_of(start + step * CHUNK, CHUNK), CHUNK)
        piece = piece_ref[source, :].astype(jnp.float32)
        left_ref[target, :] = (piece * factor_ref[...]).astype(jnp.bfloat16)


def fill(out_ref, index, tile):
    half = tile.shape[0] // 2
    rows = tile.shape[1]
    out_ref[index, :, 0:rows] = tile[:half].astype(out_ref.dtype)
    out_ref[index, :, rows : 2 * rows] = tile[half:].astype(out_ref.dtype)


def product_of(right, left):
    return lax.dot_general(right, left, (((1,), (1,)), ((), ())), preferred_element_type=jnp.float32)


def owner(far, p):
    return jnp.where(far == 1, 3 * p, 1 + p)


def tiles_kernel(late, place_ref, factor_ref, *refs):
    keep_ref, give_ref, left_ref = refs[-3:]
    pieces = refs[:-3]
    order = (0, 3, 1, 2) if late else (0, 3, 1)
    here = dict(zip((0, 3, 1, 2), pieces[:NY]))
    above = dict(zip(order, pieces[NY : NY + len(order)]))
    below = dict(zip(order, pieces[NY + len(order) :]))
    rows = pieces[0].shape[0]
    y = place_ref[0]
    c = place_ref[1]
    for plane, group in enumerate((below, here, above)):
        for rel, ref in group.items():
            scale_into(left_ref, ref, factor_ref, (plane * NY + lax.rem(y + rel, NY)) * rows)

    def left_of(r, offset, count):
        start = (lax.rem(y + r, NY) + 2 * NY - offset) * rows
        return left_ref[pl.ds(pl.multiple_of(start, CHUNK), count * rows), :]

    @pl.loop(0, 4)
    def _(turn):
        far = turn // 2
        given = lax.rem(turn, 2)
        core = jnp.where(given == 1, 1 - c, c)
        lowest = 4 * far + 2 * core + 1

        def place(slot, p, tile):
            index = slot * 4 + owner(far, p) if late else owner(far, p) * 2 + slot

            @pl.when(given == 0)
            def _():
                fill(keep_ref, index, tile)

            @pl.when(given == 1)
            def _():
                fill(give_ref, index, tile)

        first = core == 0
        if late:
            pair = product_of(above[2][...], left_of(2, lowest + 1, 2))
            place(0, 1, pair[:, :rows])
            place(0, 0, pair[:, rows:])
            right = jnp.where(first, above[3][...], above[1][...])
            place(1, 0, product_of(right, left_of(jnp.where(first, 3, 1), lowest, 1)))
            place(1, 1, product_of(above[0][...], left_of(0, lowest + 1, 1)))
        else:
            right = jnp.where(first, above[1][...], above[3][...])
            pair = product_of(right, left_of(jnp.where(first, 1, 3), lowest + 1, 2))
            place(jnp.where(first, 1, 0), 1, pair[:, :rows])
            place(1, 0, pair[:, rows:])
            right = jnp.where(first, above[3][...], above[1][...])
            place(jnp.where(first, 0, 1), 1, product_of(right, left_of(jnp.where(first, 3, 1), lowest + 1, 1)))
            place(0, 0, product_of(above[0][...], left_of(0, lowest, 1)))


def tiles(late, place, factor, here, above, below):
    order = (0, 3, 1, 2) if late else (0, 3, 1)
    arrays = [here[r] for r in (0, 3, 1, 2)] + [above[r] for r in order] + [below[r] for r in order]
    rows, width = arrays[0].shape
    half = rows // 2
    vmem = pl.BlockSpec(memory_space=pltpu.VMEM)
    keep, give = pl.pallas_call(
        functools.partial(tiles_kernel, late),
        in_specs=[pl.BlockSpec(memory_space=pltpu.SMEM)] + [vmem] * (1 + len(arrays)),
        out_specs=[vmem] * 2,
        out_shape=[
            jax.ShapeDtypeStruct((8, half, 2 * rows), jnp.float32),
            jax.ShapeDtypeStruct((8, half, 2 * rows), jnp.bfloat16),
        ],
        scratch_shapes=[pltpu.VMEM((3 * NY * rows, width), jnp.bfloat16)],
        compiler_params=pltpu.CompilerParams(vmem_limit_bytes=28 * 2**20),
        cost_estimate=pl.CostEstimate(
            flops=32 * rows * rows * width, bytes_accessed=12 * rows * width * 2, transcendentals=0
        ),
    )(place, factor, *arrays)
    shape = (2, 4, half, 2 * rows) if late else (4, 2, half, 2 * rows)
    return keep.reshape(shape), give.reshape(shape)


def local_fn(blocks):
    def flat(e, x, c):
        return (e % blocks) * 8 + (x % 4) * 2 + c

    def ring(e, by):
        return e - e % NY + (e + by) % NY

    def send(value, move):
        pairs = []
        for e in range(blocks):
            for x in range(4):
                for c in range(2):
                    target = move(e, x, c)
                    if target is not None:
                        pairs.append((flat(e, x, c), flat(*target)))
        return lax.ppermute(value, AXES, pairs)

    def offset_of(x, c):
        return (4 if x in (0, 3) else 0) + 2 * c + 1 + (1 if x >= 2 else 0)

    def local(grads, second_moment, step_size, partners, counts):
        width = grads.shape[2]
        rows = grads.shape[1]
        reach = partners.shape[1]
        quarter = width // NY
        part = rows // 4
        own = grads[0]
        e = lax.axis_index("ex")
        k = lax.axis_index("ckpt")
        y = lax.bitwise_and(e, NY - 1)
        x = lax.shift_right_logical(k, 1)
        c = lax.bitwise_and(k, 1)
        starts = [lax.bitwise_and(y + i, NY - 1) * quarter for i in range(NY)]
        spots = [lax.bitwise_and(x + i, 3) for i in range(4)]
        low = x < 2
        is_far = jnp.logical_or(x == 0, x == 3)
        offset = jnp.where(is_far, NY, 0) + 2 * c + 1 + jnp.where(low, 0, 1)
        later_block = x >= 2
        own, starts, spots, low, offset, later_block, y, c, e, zero = lax.optimization_barrier(
            (own, starts, spots, low, offset - 1, later_block, y, c, e, e - e)
        )

        def cut(block, i):
            return lax.dynamic_slice(block, (zero, starts[i]), (rows, quarter), allow_negative_indices=False)

        def pick(array, i, axis):
            at = [zero] * array.ndim
            at[axis] = spots[i % 4]
            sizes = list(array.shape)
            sizes[axis] = 1
            return lax.dynamic_slice(array, at, sizes, allow_negative_indices=False).squeeze(axis)

        here = [None] * NY
        above = [None] * NY
        below = [None] * NY
        ahead, behind = cut(own, 1), cut(own, 3)
        own, ahead, behind = lax.optimization_barrier((own, ahead, behind))
        here[0] = cut(own, 0)
        here[3] = send(ahead, lambda e, x, c: (ring(e, 1), x, c))
        here[1] = send(behind, lambda e, x, c: (ring(e, 3), x, c))
        here[2] = send(cut(own, 2), lambda e, x, c: (ring(e, 2), x, c))
        for r in (0, 3, 1, 2):
            above[r] = send(here[r], lambda e, x, c: (e - NY, x, c))
            below[r] = send(here[r], lambda e, x, c: (e + NY, x, c))

        offsets = jnp.mod(partners[0] - e, blocks)
        alive = jnp.arange(reach, dtype=jnp.int32) < counts[0]
        wanted = jnp.arange(1, reach + 1, dtype=jnp.int32)
        matched = jnp.logical_and(offsets[:, None] == wanted[None, :], alive[:, None])
        listed = jnp.sum(matched.astype(jnp.float32), axis=0)
        listed = send(listed, lambda e, x, c: (e + offset_of(x, c) - NY, x, c))
        weight = lax.dynamic_slice(listed, (offset,), (1,), allow_negative_indices=False)[0]

        factor = step_size[:, None] / (jnp.sqrt(second_moment) + EPSILON) * width ** (-0.5)
        factor = lax.dynamic_slice(factor, (zero, starts[0]), (1, quarter), allow_negative_indices=False)
        place = jnp.stack([y, c])
        keep, give = tiles(False, place, factor, here, above, below)

        def low_of(x):
            return x < 2

        def narrow(value):
            return value.astype(jnp.bfloat16)

        def wide(value):
            return value.astype(jnp.float32)

        given = send(give, lambda e, x, c: (e, x, 1 - c))
        total = keep + wide(given)
        early = pick(total, 0, 0)
        arrived_early = [send(narrow(pick(total, t, 0)), lambda e, x, c, t=t: (e, x + t, c)) for t in (1, 3, 2)]
        keep, give = tiles(True, place, factor, here, above, below)
        given = send(give, lambda e, x, c: (e, x, 1 - c))
        total = keep + wide(given)

        def rest(e, c):
            return ring(e, 3 if c == 0 else 1)

        upper, lower = total[:, :, :part], total[:, :, part:]
        by2 = send(narrow(lower[0]), lambda e, x, c: (ring(e, 2), x, c))
        by1 = send(narrow(lower[1, :2]), lambda e, x, c: (rest(e, c), x, c))
        upper_own = pick(upper, 0, 1)
        arrived = [send(narrow(pick(upper, t, 1)), lambda e, x, c, t=t: (e, x + t, c)) for t in (1, 3, 2)]
        lower_own = wide(by2) + jnp.concatenate([wide(by1), lower[1, 2:]], axis=0)
        bottom = pick(lower_own, 0, 0)
        bottom_arrived = [send(narrow(pick(lower_own, t, 0)), lambda e, x, c, t=t: (e, x + t, c)) for t in (1, 3, 2)]
        arrived_early, arrived[0] = lax.optimization_barrier((arrived_early, arrived[0]))
        for value in arrived_early:
            early = early + wide(value)
        for value in arrived:
            upper_own = upper_own + wide(value)
        ay2 = send(narrow(upper_own[0]), lambda e, x, c: (ring(e, 2), x, c))
        ey1 = send(narrow(early[1]), lambda e, x, c: (ring(e, 3 if low_of(x) and c == 1 else 1), x, c))
        padded = jnp.concatenate([upper_own[1], jnp.zeros_like(upper_own[1])], axis=0)
        mixed = send(
            narrow(jnp.where(low, padded, early[0])), lambda e, x, c: (rest(e, c) if low_of(x) else ring(e, 3), x, c)
        )
        for value in bottom_arrived:
            bottom = bottom + wide(value)
        top = wide(ay2) + jnp.where(low, 0.0, upper_own[1])
        final = jnp.concatenate([top, bottom], axis=0) + wide(ey1) + wide(mixed) + jnp.where(low, early[0], 0.0)
        final = jnp.where(weight > 0, final, 0.0)

        def deliver(first):
            def move(e, x, c):
                far = x in (0, 3)
                if (x < 2) == first:
                    return (e + NY, 0 if far else 1, 1 - c)
                return (e + NY - offset_of(x, c), 3 if far else 2, c)

            return move

        one = send(final, deliver(True))
        two = send(final, deliver(False))

        def later(tile):
            return jnp.concatenate([tile[:, :rows], tile[:, rows:]], axis=0)

        one, two = later(one), later(two)
        backward = jnp.concatenate([two, one], axis=1)
        forward = jnp.concatenate([two.T, one.T], axis=1)
        return jnp.where(later_block, forward, backward)

    return local


def build(mesh):
    local = local_fn(mesh.shape["ex"])
    in_specs = (P("ckpt", "ex", None), P("ckpt", None), P("ckpt"), P("ex", None), P("ex"))
    return jax.shard_map(local, mesh=mesh, in_specs=in_specs, out_specs=P("ex", "ckpt"), check_vma=False)


def solution(mesh):
    return build(mesh)
```

```python
import functools

import jax
import jax.numpy as jnp
from jax import lax
from jax.experimental import pallas as pl
from jax.experimental.pallas import tpu as pltpu
from jax.sharding import PartitionSpec as P


EPSILON = 1e-08
AXES = ("ex", "ckpt")
NY = 4
CHUNK = 32


def scale_into(left_ref, piece_ref, factor_ref, start):
    @pl.loop(0, piece_ref.shape[0] // CHUNK)
    def _(step):
        source = pl.ds(pl.multiple_of(step * CHUNK, CHUNK), CHUNK)
        target = pl.ds(pl.multiple_of(start + step * CHUNK, CHUNK), CHUNK)
        piece = piece_ref[source, :].astype(jnp.float32)
        left_ref[target, :] = (piece * factor_ref[...]).astype(jnp.bfloat16)


def fill(out_ref, index, tile):
    half = tile.shape[0] // 2
    rows = tile.shape[1]
    out_ref[index, :, 0:rows] = tile[:half].astype(out_ref.dtype)
    out_ref[index, :, rows : 2 * rows] = tile[half:].astype(out_ref.dtype)


def owner(far, p):
    return jnp.where(far == 1, 3 * p, 1 + p)


SCALED = {
    "prep": tuple((plane, r) for plane in (0, 1, 2) for r in (0, 3)) + ((1, 1), (1, 2)),
    "early": ((0, 1), (2, 1)),
    "late": ((0, 2), (2, 2)),
}
RIGHT = {"prep": (0, 3), "early": (0, 3, 1), "late": (0, 3, 1, 2)}


def tiles_kernel(stage, place_ref, factor_ref, *refs):
    count = len(SCALED[stage])
    scaled, refs = refs[:count], refs[count:]
    above, refs = dict(zip(RIGHT[stage], refs)), refs[len(RIGHT[stage]) :]
    left_ref, keep_ref, give_ref = refs[-3:]
    rows = scaled[0].shape[0]
    y = place_ref[0]
    c = place_ref[1]
    for (plane, rel), ref in zip(SCALED[stage], scaled):
        scale_into(left_ref, ref, factor_ref, (plane * NY + lax.rem(y + rel, NY)) * rows)

    @pl.loop(0, 2)
    def _(far):
        def product(r, offset, blocks):
            start = (lax.rem(y + r, NY) + 2 * NY - 4 * far - offset) * rows
            left = left_ref[pl.ds(pl.multiple_of(start, CHUNK), blocks * rows), :]
            return lax.dot_general(
                above[r][...], left, (((1,), (1,)), ((), ())), preferred_element_type=jnp.float32
            )

        def place(core, slot, p, tile):
            spot = owner(far, p)
            index = slot * 4 + spot if stage == "late" else spot * 2 + slot

            @pl.when(c == core)
            def _():
                fill(keep_ref, index, tile)

            @pl.when(c != core)
            def _():
                fill(give_ref, index, tile)

        if stage == "prep":
            place(0, 0, 0, product(0, 1, 1))
            pair = product(3, 4, 2)
            place(1, 0, 1, pair[:, :rows])
            place(1, 1, 0, pair[:, rows:])
        elif stage == "early":
            pair = product(1, 2, 2)
            place(0, 1, 1, pair[:, :rows])
            place(0, 1, 0, pair[:, rows:])
            place(0, 0, 1, product(3, 2, 1))
            place(1, 1, 1, product(1, 4, 1))
            place(1, 0, 0, product(0, 3, 1))
        else:
            four = product(2, 4, 4)
            for i, (core, p) in enumerate(((1, 1), (1, 0), (0, 1), (0, 0))):
                place(core, 0, p, four[:, i * rows : (i + 1) * rows])
            place(0, 1, 0, product(3, 1, 1))
            place(1, 1, 0, product(1, 3, 1))
            place(0, 1, 1, product(0, 2, 1))
            place(1, 1, 1, product(0, 4, 1))


def tiles(stage, place, factor, pieces, carried):
    _, _, above = pieces
    arrays = [pieces[plane][r] for plane, r in SCALED[stage]] + [above[r] for r in RIGHT[stage]]
    rows, width = arrays[0].shape
    half = rows // 2
    vmem = pl.BlockSpec(memory_space=pltpu.VMEM)
    first = 2 + len(arrays)
    partial = jax.ShapeDtypeStruct((8, half, 2 * rows), jnp.float32)
    return pl.pallas_call(
        functools.partial(tiles_kernel, stage),
        in_specs=[pl.BlockSpec(memory_space=pltpu.SMEM)] + [vmem] * (1 + len(arrays) + len(carried)),
        out_specs=[vmem] * 3,
        out_shape=[jax.ShapeDtypeStruct((3 * NY * rows, width), jnp.bfloat16), partial, partial],
        input_output_aliases={first + i: i for i in range(len(carried))},
        compiler_params=pltpu.CompilerParams(vmem_limit_bytes=24 * 2**20),
        cost_estimate=pl.CostEstimate(
            flops=20 * rows * rows * width, bytes_accessed=12 * rows * width * 2, transcendentals=0
        ),
    )(place, factor, *arrays, *carried)


def local_fn(blocks):
    def flat(e, x, c):
        return (e % blocks) * 8 + (x % 4) * 2 + c

    def ring(e, by):
        return e - e % NY + (e + by) % NY

    def send(value, move):
        pairs = []
        for e in range(blocks):
            for x in range(4):
                for c in range(2):
                    target = move(e, x, c)
                    if target is not None:
                        pairs.append((flat(e, x, c), flat(*target)))
        return lax.ppermute(value, AXES, pairs)

    def offset_of(x, c):
        return (4 if x in (0, 3) else 0) + 2 * c + 1 + (1 if x >= 2 else 0)

    def local(grads, second_moment, step_size, partners, counts):
        width = grads.shape[2]
        rows = grads.shape[1]
        reach = partners.shape[1]
        quarter = width // NY
        part = rows // 4
        own = grads[0]
        e = lax.axis_index("ex")
        k = lax.axis_index("ckpt")
        y = lax.bitwise_and(e, NY - 1)
        x = lax.shift_right_logical(k, 1)
        c = lax.bitwise_and(k, 1)
        starts = [lax.bitwise_and(y + i, NY - 1) * quarter for i in range(NY)]
        spots = [lax.bitwise_and(x + i, 3) for i in range(4)]
        low = x < 2
        is_far = jnp.logical_or(x == 0, x == 3)
        offset = jnp.where(is_far, NY, 0) + 2 * c + 1 + jnp.where(low, 0, 1)
        later_block = x >= 2
        own, starts, spots, low, offset, later_block, y, c, e, zero = lax.optimization_barrier(
            (own, starts, spots, low, offset - 1, later_block, y, c, e, e - e)
        )

        def cut(block, i):
            return lax.dynamic_slice(block, (zero, starts[i]), (rows, quarter), allow_negative_indices=False)

        def pick(array, i, axis):
            at = [zero] * array.ndim
            at[axis] = spots[i % 4]
            sizes = list(array.shape)
            sizes[axis] = 1
            return lax.dynamic_slice(array, at, sizes, allow_negative_indices=False).squeeze(axis)

        here = [None] * NY
        above = [None] * NY
        below = [None] * NY
        ahead, behind = cut(own, 1), cut(own, 3)
        own, ahead, behind = lax.optimization_barrier((own, ahead, behind))
        here[0] = cut(own, 0)
        here[3] = send(ahead, lambda e, x, c: (ring(e, 1), x, c))
        here[1] = send(behind, lambda e, x, c: (ring(e, 3), x, c))
        here[2] = send(cut(own, 2), lambda e, x, c: (ring(e, 2), x, c))
        for r in (0, 3, 1, 2):
            above[r] = send(here[r], lambda e, x, c: (e - NY, x, c))
            below[r] = send(here[r], lambda e, x, c: (e + NY, x, c))

        offsets = jnp.mod(partners[0] - e, blocks)
        alive = jnp.arange(reach, dtype=jnp.int32) < counts[0]
        wanted = jnp.arange(1, reach + 1, dtype=jnp.int32)
        matched = jnp.logical_and(offsets[:, None] == wanted[None, :], alive[:, None])
        listed = jnp.sum(matched.astype(jnp.float32), axis=0)
        listed = send(listed, lambda e, x, c: (e + offset_of(x, c) - NY, x, c))
        weight = lax.dynamic_slice(listed, (offset,), (1,), allow_negative_indices=False)[0]

        factor = step_size[:, None] / (jnp.sqrt(second_moment) + EPSILON) * width ** (-0.5)
        factor = lax.dynamic_slice(factor, (zero, starts[0]), (1, quarter), allow_negative_indices=False)
        place = jnp.stack([y, c])
        pieces = (below, here, above)
        carried = tiles("prep", place, factor, pieces, ())
        left, keep, give = tiles("early", place, factor, pieces, carried)
        keep, give = (value.reshape(4, 2, rows // 2, 2 * rows) for value in (keep, give))

        def low_of(x):
            return x < 2

        def narrow(value):
            return value.astype(jnp.bfloat16)

        def wide(value):
            return value.astype(jnp.float32)

        total = keep + send(give, lambda e, x, c: (e, x, 1 - c))
        early = pick(total, 0, 0)
        arrived_early = [send(narrow(pick(total, t, 0)), lambda e, x, c, t=t: (e, x + t, c)) for t in (1, 3, 2)]
        left, keep, give = tiles("late", place, factor, pieces, (left,))
        keep, give = (value.reshape(2, 4, rows // 2, 2 * rows) for value in (keep, give))
        total = keep + send(give, lambda e, x, c: (e, x, 1 - c))

        def rest(e, c):
            return ring(e, 3 if c == 0 else 1)

        upper, lower = total[:, :, :part], total[:, :, part:]
        by2 = send(narrow(lower[0]), lambda e, x, c: (ring(e, 2), x, c))
        by1 = send(narrow(lower[1, :2]), lambda e, x, c: (rest(e, c), x, c))
        upper_own = pick(upper, 0, 1)
        arrived = [send(narrow(pick(upper, t, 1)), lambda e, x, c, t=t: (e, x + t, c)) for t in (1, 3, 2)]
        lower_own = wide(by2) + jnp.concatenate([wide(by1), lower[1, 2:]], axis=0)
        bottom = pick(lower_own, 0, 0)
        bottom_arrived = [send(narrow(pick(lower_own, t, 0)), lambda e, x, c, t=t: (e, x + t, c)) for t in (1, 3, 2)]
        arrived_early, arrived[0] = lax.optimization_barrier((arrived_early, arrived[0]))
        for value in arrived_early:
            early = early + wide(value)
        for value in arrived:
            upper_own = upper_own + wide(value)
        ay2 = send(narrow(upper_own[0]), lambda e, x, c: (ring(e, 2), x, c))
        ey1 = send(narrow(early[1]), lambda e, x, c: (ring(e, 3 if low_of(x) and c == 1 else 1), x, c))
        padded = jnp.concatenate([upper_own[1], jnp.zeros_like(upper_own[1])], axis=0)
        mixed = send(
            narrow(jnp.where(low, padded, early[0])), lambda e, x, c: (rest(e, c) if low_of(x) else ring(e, 3), x, c)
        )
        for value in bottom_arrived:
            bottom = bottom + wide(value)
        top = wide(ay2) + jnp.where(low, 0.0, upper_own[1])
        final = jnp.concatenate([top, bottom], axis=0) + wide(ey1) + wide(mixed) + jnp.where(low, early[0], 0.0)
        final = narrow(jnp.where(weight > 0, final, 0.0))

        def deliver(first):
            def move(e, x, c):
                far = x in (0, 3)
                if (x < 2) == first:
                    return (e + NY, 0 if far else 1, 1 - c)
                return (e + NY - offset_of(x, c), 3 if far else 2, c)

            return move

        one = send(final, deliver(True))
        two = send(final, deliver(False))

        def later(tile):
            return jnp.concatenate([tile[:, :rows], tile[:, rows:]], axis=0)

        one, two = later(wide(one)), later(wide(two))
        backward = jnp.concatenate([two, one], axis=1)
        forward = jnp.concatenate([two.T, one.T], axis=1)
        return jnp.where(later_block, forward, backward)

    return local


def build(mesh):
    local = local_fn(mesh.shape["ex"])
    in_specs = (P("ckpt", "ex", None), P("ckpt", None), P("ckpt"), P("ex", None), P("ex"))
    return jax.shard_map(local, mesh=mesh, in_specs=in_specs, out_specs=P("ex", "ckpt"), check_vma=False)


def solution(mesh):
    return build(mesh)
```

```python
import functools

import jax
import jax.numpy as jnp
from jax import lax
from jax.experimental import pallas as pl
from jax.experimental.pallas import tpu as pltpu
from jax.sharding import PartitionSpec as P


EPSILON = 1e-08
AXES = ("ex", "ckpt")
NY = 4
CHUNK = 32


def scale_into(left_ref, piece_ref, factor_ref, start):
    @pl.loop(0, piece_ref.shape[0] // CHUNK)
    def _(step):
        source = pl.ds(pl.multiple_of(step * CHUNK, CHUNK), CHUNK)
        target = pl.ds(pl.multiple_of(start + step * CHUNK, CHUNK), CHUNK)
        piece = piece_ref[source, :].astype(jnp.float32)
        left_ref[target, :] = (piece * factor_ref[...]).astype(jnp.bfloat16)


def fill(out_ref, index, tile):
    half = tile.shape[0] // 2
    rows = tile.shape[1]
    out_ref[index, :, 0:rows] = tile[:half].astype(out_ref.dtype)
    out_ref[index, :, rows : 2 * rows] = tile[half:].astype(out_ref.dtype)


def owner(far, p):
    return jnp.where(far == 1, 3 * p, 1 + p)


SCALED = {
    "prep": tuple((plane, r) for plane in (0, 1, 2) for r in (0, 3)) + ((1, 1),),
    "early": ((0, 1), (2, 1)),
    "mid": ((1, 2),),
    "late": ((0, 2), (2, 2)),
}
RIGHT = {"prep": (0, 3), "early": (0, 3, 1), "mid": (0, 3, 1), "late": (0, 3, 1, 2)}
SPLIT = ((0, 0, 3, 1), (1, 0, 1, 3), (0, 1, 0, 2))


def tiles_kernel(stage, place_ref, factor_ref, *refs):
    count = len(SCALED[stage])
    scaled, refs = refs[:count], refs[count:]
    above, refs = dict(zip(RIGHT[stage], refs)), refs[len(RIGHT[stage]) :]
    left_ref, keep_ref, give_ref = refs[-3:]
    rows = scaled[0].shape[0]
    y = place_ref[0]
    c = place_ref[1]
    for (plane, rel), ref in zip(SCALED[stage], scaled):
        scale_into(left_ref, ref, factor_ref, (plane * NY + lax.rem(y + rel, NY)) * rows)

    def product(far, r, offset, blocks):
        start = (lax.rem(y + r, NY) + 2 * NY - 4 * far - offset) * rows
        left = left_ref[pl.ds(pl.multiple_of(start, CHUNK), blocks * rows), :]
        return lax.dot_general(above[r][...], left, (((1,), (1,)), ((), ())), preferred_element_type=jnp.float32)

    def place(far, core, slot, p, tile):
        spot = owner(far, p)
        index = spot * 2 + slot if stage in ("prep", "early") else slot * 4 + spot

        @pl.when(c == core)
        def _():
            fill(keep_ref, index, tile)

        @pl.when(c != core)
        def _():
            fill(give_ref, index, tile)

    @pl.loop(0, 2)
    def _(far):
        if stage == "prep":
            place(far, 0, 0, 0, product(far, 0, 1, 1))
            pair = product(far, 3, 4, 2)
            place(far, 1, 0, 1, pair[:, :rows])
            place(far, 1, 1, 0, pair[:, rows:])
        elif stage == "early":
            pair = product(far, 1, 2, 2)
            place(far, 0, 1, 1, pair[:, :rows])
            place(far, 0, 1, 0, pair[:, rows:])
            place(far, 0, 0, 1, product(far, 3, 2, 1))
            place(far, 1, 1, 1, product(far, 1, 4, 1))
            place(far, 1, 0, 0, product(far, 0, 3, 1))
        elif stage == "mid":
            place(far, 1, 1, 1, product(far, 0, 4, 1))
        else:
            four = product(far, 2, 4, 4)
            for i, (core, p) in enumerate(((1, 1), (1, 0), (0, 1), (0, 0))):
                place(far, core, 0, p, four[:, i * rows : (i + 1) * rows])

    if stage in ("mid", "late"):
        for core, p, r, offset in SPLIT:
            far = jnp.where(lax.rem(y + r, NY) < offset, 0, 1)
            far = 1 - far if stage == "late" else far
            place(far, core, 1, p, product(far, r, offset, 1))


def tiles(stage, place, factor, pieces, carried):
    _, _, above = pieces
    arrays = [pieces[plane][r] for plane, r in SCALED[stage]] + [above[r] for r in RIGHT[stage]]
    rows, width = arrays[0].shape
    half = rows // 2
    vmem = pl.BlockSpec(memory_space=pltpu.VMEM)
    first = 2 + len(arrays)
    partial = jax.ShapeDtypeStruct((8, half, 2 * rows), jnp.float32)
    return pl.pallas_call(
        functools.partial(tiles_kernel, stage),
        in_specs=[pl.BlockSpec(memory_space=pltpu.SMEM)] + [vmem] * (1 + len(arrays) + len(carried)),
        out_specs=[vmem] * 3,
        out_shape=[jax.ShapeDtypeStruct((3 * NY * rows, width), jnp.bfloat16), partial, partial],
        input_output_aliases={first + i: i for i in range(len(carried))},
        compiler_params=pltpu.CompilerParams(vmem_limit_bytes=24 * 2**20),
        cost_estimate=pl.CostEstimate(
            flops=20 * rows * rows * width, bytes_accessed=12 * rows * width * 2, transcendentals=0
        ),
    )(place, factor, *arrays, *carried)


def local_fn(blocks):
    def flat(e, x, c):
        return (e % blocks) * 8 + (x % 4) * 2 + c

    def ring(e, by):
        return e - e % NY + (e + by) % NY

    def send(value, move):
        pairs = []
        for e in range(blocks):
            for x in range(4):
                for c in range(2):
                    target = move(e, x, c)
                    if target is not None:
                        pairs.append((flat(e, x, c), flat(*target)))
        return lax.ppermute(value, AXES, pairs)

    def offset_of(x, c):
        return (4 if x in (0, 3) else 0) + 2 * c + 1 + (1 if x >= 2 else 0)

    def local(grads, second_moment, step_size, partners, counts):
        width = grads.shape[2]
        rows = grads.shape[1]
        reach = partners.shape[1]
        quarter = width // NY
        part = rows // 4
        own = grads[0]
        e = lax.axis_index("ex")
        k = lax.axis_index("ckpt")
        y = lax.bitwise_and(e, NY - 1)
        x = lax.shift_right_logical(k, 1)
        c = lax.bitwise_and(k, 1)
        starts = [lax.bitwise_and(y + i, NY - 1) * quarter for i in range(NY)]
        spots = [lax.bitwise_and(x + i, 3) for i in range(4)]
        low = x < 2
        is_far = jnp.logical_or(x == 0, x == 3)
        offset = jnp.where(is_far, NY, 0) + 2 * c + 1 + jnp.where(low, 0, 1)
        later_block = x >= 2
        own, starts, spots, low, offset, later_block, y, c, e, zero = lax.optimization_barrier(
            (own, starts, spots, low, offset - 1, later_block, y, c, e, e - e)
        )

        def cut(block, i):
            return lax.dynamic_slice(block, (zero, starts[i]), (rows, quarter), allow_negative_indices=False)

        def pick(array, i, axis):
            at = [zero] * array.ndim
            at[axis] = spots[i % 4]
            sizes = list(array.shape)
            sizes[axis] = 1
            return lax.dynamic_slice(array, at, sizes, allow_negative_indices=False).squeeze(axis)

        here = [None] * NY
        above = [None] * NY
        below = [None] * NY
        ahead, behind = cut(own, 1), cut(own, 3)
        own, ahead, behind = lax.optimization_barrier((own, ahead, behind))
        here[0] = cut(own, 0)
        here[3] = send(ahead, lambda e, x, c: (ring(e, 1), x, c))
        here[1] = send(behind, lambda e, x, c: (ring(e, 3), x, c))
        here[2] = send(cut(own, 2), lambda e, x, c: (ring(e, 2), x, c))
        for r in (0, 3, 1, 2):
            above[r] = send(here[r], lambda e, x, c: (e - NY, x, c))
            below[r] = send(here[r], lambda e, x, c: (e + NY, x, c))

        offsets = jnp.mod(partners[0] - e, blocks)
        alive = jnp.arange(reach, dtype=jnp.int32) < counts[0]
        wanted = jnp.arange(1, reach + 1, dtype=jnp.int32)
        matched = jnp.logical_and(offsets[:, None] == wanted[None, :], alive[:, None])
        listed = jnp.sum(matched.astype(jnp.float32), axis=0)
        listed = send(listed, lambda e, x, c: (e + offset_of(x, c) - NY, x, c))
        weight = lax.dynamic_slice(listed, (offset,), (1,), allow_negative_indices=False)[0]

        factor = step_size[:, None] / (jnp.sqrt(second_moment) + EPSILON) * width ** (-0.5)
        factor = lax.dynamic_slice(factor, (zero, starts[0]), (1, quarter), allow_negative_indices=False)
        place = jnp.stack([y, c])
        pieces = (below, here, above)
        carried = tiles("prep", place, factor, pieces, ())
        left, keep, give = tiles("early", place, factor, pieces, carried)
        carried = tiles("mid", place, factor, pieces, (left,))
        keep, give = (value.reshape(4, 2, rows // 2, 2 * rows) for value in (keep, give))

        def low_of(x):
            return x < 2

        def narrow(value):
            return value.astype(jnp.bfloat16)

        def wide(value):
            return value.astype(jnp.float32)

        total = keep + send(give, lambda e, x, c: (e, x, 1 - c))
        early = pick(total, 0, 0)
        arrived_early = [send(narrow(pick(total, t, 0)), lambda e, x, c, t=t: (e, x + t, c)) for t in (1, 3, 2)]
        left, keep, give = tiles("late", place, factor, pieces, carried)
        keep, give = (value.reshape(2, 4, rows // 2, 2 * rows) for value in (keep, give))
        total = keep + send(give, lambda e, x, c: (e, x, 1 - c))

        def rest(e, c):
            return ring(e, 3 if c == 0 else 1)

        upper, lower = total[:, :, :part], total[:, :, part:]
        by2 = send(narrow(lower[0]), lambda e, x, c: (ring(e, 2), x, c))
        by1 = send(narrow(lower[1, :2]), lambda e, x, c: (rest(e, c), x, c))
        upper_own = pick(upper, 0, 1)
        arrived = [send(narrow(pick(upper, t, 1)), lambda e, x, c, t=t: (e, x + t, c)) for t in (1, 3, 2)]
        lower_own = wide(by2) + jnp.concatenate([wide(by1), lower[1, 2:]], axis=0)
        bottom = pick(lower_own, 0, 0)
        bottom_arrived = [send(narrow(pick(lower_own, t, 0)), lambda e, x, c, t=t: (e, x + t, c)) for t in (1, 3, 2)]
        arrived_early, arrived[0] = lax.optimization_barrier((arrived_early, arrived[0]))
        for value in arrived_early:
            early = early + wide(value)
        for value in arrived:
            upper_own = upper_own + wide(value)
        ay2 = send(narrow(upper_own[0]), lambda e, x, c: (ring(e, 2), x, c))
        ey1 = send(narrow(early[1]), lambda e, x, c: (ring(e, 3 if low_of(x) and c == 1 else 1), x, c))
        padded = jnp.concatenate([upper_own[1], jnp.zeros_like(upper_own[1])], axis=0)
        mixed = send(
            narrow(jnp.where(low, padded, early[0])), lambda e, x, c: (rest(e, c) if low_of(x) else ring(e, 3), x, c)
        )
        for value in bottom_arrived:
            bottom = bottom + wide(value)
        top = wide(ay2) + jnp.where(low, 0.0, upper_own[1])
        final = jnp.concatenate([top, bottom], axis=0) + wide(ey1) + wide(mixed) + jnp.where(low, early[0], 0.0)
        final = narrow(jnp.where(weight > 0, final, 0.0))

        def deliver(first):
            def move(e, x, c):
                far = x in (0, 3)
                if (x < 2) == first:
                    return (e + NY, 0 if far else 1, 1 - c)
                return (e + NY - offset_of(x, c), 3 if far else 2, c)

            return move

        one = send(final, deliver(True))
        two = send(final, deliver(False))

        def later(tile):
            return jnp.concatenate([tile[:, :rows], tile[:, rows:]], axis=0)

        one, two = later(wide(one)), later(wide(two))
        backward = jnp.concatenate([two, one], axis=1)
        forward = jnp.concatenate([two.T, one.T], axis=1)
        return jnp.where(later_block, forward, backward)

    return local


def build(mesh):
    local = local_fn(mesh.shape["ex"])
    in_specs = (P("ckpt", "ex", None), P("ckpt", None), P("ckpt"), P("ex", None), P("ex"))
    return jax.shard_map(local, mesh=mesh, in_specs=in_specs, out_specs=P("ex", "ckpt"), check_vma=False)


def solution(mesh):
    return build(mesh)
```

```python
import functools

import jax
import jax.numpy as jnp
from jax import lax
from jax.experimental import pallas as pl
from jax.experimental.pallas import tpu as pltpu
from jax.sharding import PartitionSpec as P


EPSILON = 1e-08
AXES = ("ex", "ckpt")
NY = 4
CHUNK = 32


def scale_into(left_ref, piece_ref, factor_ref, start):
    @pl.loop(0, piece_ref.shape[0] // CHUNK)
    def _(step):
        source = pl.ds(pl.multiple_of(step * CHUNK, CHUNK), CHUNK)
        target = pl.ds(pl.multiple_of(start + step * CHUNK, CHUNK), CHUNK)
        piece = piece_ref[source, :].astype(jnp.float32)
        left_ref[target, :] = (piece * factor_ref[...]).astype(jnp.bfloat16)


def fill(out_ref, index, tile):
    half = tile.shape[0] // 2
    rows = tile.shape[1]
    out_ref[index, :, 0:rows] = tile[:half].astype(out_ref.dtype)
    out_ref[index, :, rows : 2 * rows] = tile[half:].astype(out_ref.dtype)


def owner(far, p):
    return jnp.where(far == 1, 3 * p, 1 + p)


SCALED = {
    "prep": tuple((plane, r) for plane in (0, 1, 2) for r in (0, 3)) + ((1, 1),),
    "early": ((0, 1), (2, 1)),
    "mid": ((1, 2),),
    "late": ((0, 2), (2, 2)),
}
RIGHT = {"prep": (0, 3), "early": (0, 3, 1), "mid": (0, 3, 1), "late": (0, 3, 1, 2)}
SPLIT = ((0, 0, 3, 1), (1, 0, 1, 3), (0, 1, 0, 2))


def tiles_kernel(stage, place_ref, factor_ref, *refs):
    count = len(SCALED[stage])
    scaled, refs = refs[:count], refs[count:]
    above, refs = dict(zip(RIGHT[stage], refs)), refs[len(RIGHT[stage]) :]
    left_ref, keep_ref, give_ref = refs[-3:]
    rows = scaled[0].shape[0]
    y = place_ref[0]
    c = place_ref[1]
    for (plane, rel), ref in zip(SCALED[stage], scaled):
        scale_into(left_ref, ref, factor_ref, (plane * NY + lax.rem(y + rel, NY)) * rows)

    def product(far, r, offset, blocks):
        start = (lax.rem(y + r, NY) + 2 * NY - 4 * far - offset) * rows
        left = left_ref[pl.ds(pl.multiple_of(start, CHUNK), blocks * rows), :]
        return lax.dot_general(above[r][...], left, (((1,), (1,)), ((), ())), preferred_element_type=jnp.float32)

    def place(far, core, slot, p, tile):
        spot = owner(far, p)
        index = slot * 4 + spot

        @pl.when(c == core)
        def _():
            fill(keep_ref, index, tile)

        @pl.when(c != core)
        def _():
            fill(give_ref, index, tile)

    @pl.loop(0, 2)
    def _(far):
        if stage == "prep":
            place(far, 0, 0, 0, product(far, 0, 1, 1))
            pair = product(far, 3, 4, 2)
            place(far, 1, 0, 1, pair[:, :rows])
            place(far, 1, 1, 0, pair[:, rows:])
        elif stage == "early":
            pair = product(far, 1, 2, 2)
            place(far, 0, 1, 1, pair[:, :rows])
            place(far, 0, 1, 0, pair[:, rows:])
            place(far, 0, 0, 1, product(far, 3, 2, 1))
            place(far, 1, 1, 1, product(far, 1, 4, 1))
            place(far, 1, 0, 0, product(far, 0, 3, 1))
        elif stage == "mid":
            place(far, 1, 1, 1, product(far, 0, 4, 1))
        else:
            four = product(far, 2, 4, 4)
            for i, (core, p) in enumerate(((1, 1), (1, 0), (0, 1), (0, 0))):
                place(far, core, 0, p, four[:, i * rows : (i + 1) * rows])

    if stage in ("mid", "late"):
        for core, p, r, offset in SPLIT:
            far = jnp.where(lax.rem(y + r, NY) < offset, 0, 1)
            far = 1 - far if stage == "late" else far
            place(far, core, 1, p, product(far, r, offset, 1))


def tiles(stage, place, factor, pieces, carried):
    _, _, above = pieces
    arrays = [pieces[plane][r] for plane, r in SCALED[stage]] + [above[r] for r in RIGHT[stage]]
    rows, width = arrays[0].shape
    half = rows // 2
    vmem = pl.BlockSpec(memory_space=pltpu.VMEM)
    first = 2 + len(arrays)
    partial = jax.ShapeDtypeStruct((8, half, 2 * rows), jnp.float32)
    return pl.pallas_call(
        functools.partial(tiles_kernel, stage),
        in_specs=[pl.BlockSpec(memory_space=pltpu.SMEM)] + [vmem] * (1 + len(arrays) + len(carried)),
        out_specs=[vmem] * 3,
        out_shape=[jax.ShapeDtypeStruct((3 * NY * rows, width), jnp.bfloat16), partial, partial],
        input_output_aliases={first + i: i for i in range(len(carried))},
        compiler_params=pltpu.CompilerParams(vmem_limit_bytes=24 * 2**20),
        cost_estimate=pl.CostEstimate(
            flops=20 * rows * rows * width, bytes_accessed=12 * rows * width * 2, transcendentals=0
        ),
    )(place, factor, *arrays, *carried)


def local_fn(blocks):
    def flat(e, x, c):
        return (e % blocks) * 8 + (x % 4) * 2 + c

    def ring(e, by):
        return e - e % NY + (e + by) % NY

    def send(value, move):
        pairs = []
        for e in range(blocks):
            for x in range(4):
                for c in range(2):
                    target = move(e, x, c)
                    if target is not None:
                        pairs.append((flat(e, x, c), flat(*target)))
        return lax.ppermute(value, AXES, pairs)

    def offset_of(x, c):
        return (4 if x in (0, 3) else 0) + 2 * c + 1 + (1 if x >= 2 else 0)

    def local(grads, second_moment, step_size, partners, counts):
        width = grads.shape[2]
        rows = grads.shape[1]
        reach = partners.shape[1]
        quarter = width // NY
        part = rows * 3 // 10
        own = grads[0]
        e = lax.axis_index("ex")
        k = lax.axis_index("ckpt")
        y = lax.bitwise_and(e, NY - 1)
        x = lax.shift_right_logical(k, 1)
        c = lax.bitwise_and(k, 1)
        starts = [lax.bitwise_and(y + i, NY - 1) * quarter for i in range(NY)]
        spots = [lax.bitwise_and(x + i, 3) for i in range(4)]
        low = x < 2
        is_far = jnp.logical_or(x == 0, x == 3)
        offset = jnp.where(is_far, NY, 0) + 2 * c + 1 + jnp.where(low, 0, 1)
        later_block = x >= 2
        own, starts, spots, low, offset, later_block, y, c, e, zero = lax.optimization_barrier(
            (own, starts, spots, low, offset - 1, later_block, y, c, e, e - e)
        )

        def cut(block, i):
            return lax.dynamic_slice(block, (zero, starts[i]), (rows, quarter), allow_negative_indices=False)

        def pick(array, i, axis):
            at = [zero] * array.ndim
            at[axis] = spots[i % 4]
            sizes = list(array.shape)
            sizes[axis] = 1
            return lax.dynamic_slice(array, at, sizes, allow_negative_indices=False).squeeze(axis)

        here = [None] * NY
        above = [None] * NY
        below = [None] * NY
        ahead, behind = cut(own, 1), cut(own, 3)
        own, ahead, behind = lax.optimization_barrier((own, ahead, behind))
        here[0] = cut(own, 0)
        here[3] = send(ahead, lambda e, x, c: (ring(e, 1), x, c))
        here[1] = send(behind, lambda e, x, c: (ring(e, 3), x, c))
        here[2] = send(cut(own, 2), lambda e, x, c: (ring(e, 2), x, c))
        for r in (0, 3, 1, 2):
            above[r] = send(here[r], lambda e, x, c: (e - NY, x, c))
            below[r] = send(here[r], lambda e, x, c: (e + NY, x, c))

        offsets = jnp.mod(partners[0] - e, blocks)
        alive = jnp.arange(reach, dtype=jnp.int32) < counts[0]
        wanted = jnp.arange(1, reach + 1, dtype=jnp.int32)
        matched = jnp.logical_and(offsets[:, None] == wanted[None, :], alive[:, None])
        listed = jnp.sum(matched.astype(jnp.float32), axis=0)
        listed = send(listed, lambda e, x, c: (e + offset_of(x, c) - NY, x, c))
        weight = lax.dynamic_slice(listed, (offset,), (1,), allow_negative_indices=False)[0]

        factor = step_size[:, None] / (jnp.sqrt(second_moment) + EPSILON) * width ** (-0.5)
        factor = lax.dynamic_slice(factor, (zero, starts[0]), (1, quarter), allow_negative_indices=False)
        place = jnp.stack([y, c])
        pieces = (below, here, above)
        carried = tiles("prep", place, factor, pieces, ())
        left, keep, give = tiles("early", place, factor, pieces, carried)
        carried = tiles("mid", place, factor, pieces, (left,))
        keep, give = (value.reshape(2, 4, rows // 2, 2 * rows) for value in (keep, give))

        def low_of(x):
            return x < 2

        def pick_both(array, i):
            return jnp.stack([pick(array[0], i, 0), pick(array[1], i, 0)])

        def narrow(value):
            return value.astype(jnp.bfloat16)

        def wide(value):
            return value.astype(jnp.float32)

        total = keep + send(give, lambda e, x, c: (e, x, 1 - c))
        early = total
        left, keep, give = tiles("late", place, factor, pieces, carried)
        keep, give = (value.reshape(2, 4, rows // 2, 2 * rows) for value in (keep, give))
        total = keep + send(give, lambda e, x, c: (e, x, 1 - c))

        def rest(e, c):
            return ring(e, 3 if c == 0 else 1)

        upper, lower = early[:, :, :part], early[:, :, part:]
        early_upper = pick_both(upper, 0)
        arrived_early = [send(narrow(pick_both(upper, t)), lambda e, x, c, t=t: (e, x + t, c)) for t in (1, 3, 2)]
        ea = send(narrow(lower[1, :2]), lambda e, x, c: (ring(e, 1 if c == 0 else 3), x, c))
        eb = send(narrow(lower[1, 2:]), lambda e, x, c: (ring(e, 1), x, c))
        ec = send(narrow(lower[0, 2:]), lambda e, x, c: (ring(e, 3), x, c))
        early_home = lower[0, :2]

        upper, lower = total[:, :, :part], total[:, :, part:]
        by2 = send(narrow(lower[0]), lambda e, x, c: (ring(e, 2), x, c))
        by1 = send(narrow(lower[1, :2]), lambda e, x, c: (rest(e, c), x, c))
        upper_own = pick_both(upper, 0)
        arrived = [send(narrow(pick_both(upper, t)), lambda e, x, c, t=t: (e, x + t, c)) for t in (1, 3, 2)]
        ea, eb, ec, by2 = lax.optimization_barrier((ea, eb, ec, by2))
        lower_own = wide(by2) + jnp.concatenate([wide(by1), lower[1, 2:]], axis=0)
        lower_own = lower_own + jnp.concatenate([early_home + wide(ea), wide(eb) + wide(ec)], axis=0)
        bottom = pick(lower_own, 0, 0)
        bottom_arrived = [send(narrow(pick(lower_own, t, 0)), lambda e, x, c, t=t: (e, x + t, c)) for t in (1, 3, 2)]
        arrived_early, arrived[0] = lax.optimization_barrier((arrived_early, arrived[0]))
        for value in arrived_early:
            early_upper = early_upper + wide(value)
        ey1 = send(narrow(early_upper[1]), lambda e, x, c: (ring(e, 3 if low_of(x) and c == 1 else 1), x, c))
        for value in arrived:
            upper_own = upper_own + wide(value)
        ay2 = send(narrow(upper_own[0]), lambda e, x, c: (ring(e, 2), x, c))
        mixed = send(
            narrow(jnp.where(low, upper_own[1], early_upper[0])),
            lambda e, x, c: (rest(e, c) if low_of(x) else ring(e, 3), x, c),
        )
        for value in bottom_arrived:
            bottom = bottom + wide(value)
        top = jnp.where(low, early_upper[0], upper_own[1]) + wide(ey1) + wide(ay2) + wide(mixed)
        final = jnp.concatenate([top, bottom], axis=0)
        final = narrow(jnp.where(weight > 0, final, 0.0))

        def deliver(first):
            def move(e, x, c):
                far = x in (0, 3)
                if (x < 2) == first:
                    return (e + NY, 0 if far else 1, 1 - c)
                return (e + NY - offset_of(x, c), 3 if far else 2, c)

            return move

        one = send(final, deliver(True))
        two = send(final, deliver(False))

        def later(tile):
            return jnp.concatenate([tile[:, :rows], tile[:, rows:]], axis=0)

        one, two = later(wide(one)), later(wide(two))
        backward = jnp.concatenate([two, one], axis=1)
        forward = jnp.concatenate([two.T, one.T], axis=1)
        return jnp.where(later_block, forward, backward)

    return local


def build(mesh):
    local = local_fn(mesh.shape["ex"])
    in_specs = (P("ckpt", "ex", None), P("ckpt", None), P("ckpt"), P("ex", None), P("ex"))
    return jax.shard_map(local, mesh=mesh, in_specs=in_specs, out_specs=P("ex", "ckpt"), check_vma=False)


def solution(mesh):
    return build(mesh)
```
